32 devices in a mesh: graph: 8 (over z, y), feat: 4 (over x, core).
Axes of the slice: x: 2, y: 2, z: 4, core: 2. Of those that a mesh axis runs over, the one named last changes fastest.
Arguments:
- node_feats: bfloat16 [2560, 512], P(('graph', 'feat')), may hold values from -6 to 6
- edge_feats: bfloat16 [16384, 512], P(('graph', 'feat')), may hold values from -6 to 6
- senders: int32 [16384], P(('graph', 'feat')), may hold values from 0 to 319
- receiver_ref: int32 [16384], P(('graph', 'feat')), may hold values from 0 to 1087, as said below
- send_list: int32 [8, 8, 96], P('graph'), may hold values from 0 to 319, as said below
- edge_count: int32 [8], P('graph'), may hold values from 1024 to 2048, as said below
- edge_w1: bfloat16 [1536, 512], replicated, may hold values from -0.15625 to 0.15625
- edge_w2: bfloat16 [512, 512], replicated, may hold values from -0.25 to 0.25
- edge_gain: bfloat16 [512], replicated, may hold values from 0.099609375 to 1.8984375
- edge_shift: bfloat16 [512], replicated, may hold values from -3 to 3
- node_w1: bfloat16 [1024, 512], replicated, may hold values from -0.1875 to 0.1875
- node_w2: bfloat16 [512, 512], replicated, may hold values from -0.25 to 0.25
- node_gain: bfloat16 [512], replicated, may hold values from 0.099609375 to 1.8984375
- node_shift: bfloat16 [512], replicated, may hold values from -3 to 3
Outputs:
- new_edges: bfloat16 [16384, 512], P(('graph', 'feat'))
- new_nodes: bfloat16 [2560, 512], P(('graph', 'feat'))
The draws below stay inside these ranges and needn't reach their ends.
Inputs may be any that keep to these rules, and one draw needn't show every extreme that they name: `senders`: local node indices of the edge's own region. `receiver_ref`: A value below 320 is a node of the edge's own region. Otherwise q = value - 320 names slot q % 96 of the list that region s = q // 96 keeps for the edge's region; s is never the edge's own region, and when s is more than 2 steps away around the region order (either direction, wrapping) the slot is below 16. In every draw each region has an edge on slot 95 of the next region and an edge on slot 15 of the region 3 steps on. Each list send_list[s, g] holds 96 distinct local node indices of region s. Region g's live edges are its first edge_count[g] edge slots; some region has all 2048 live.
All inputs are finite; a program needn't handle non-finite values.
Results may differ from the reference program's by a relative error of at most 0.009.
Values may be sent and summed in bfloat16 or wider, within the bound.
A program may use at most 128 MiB of HBM per device.

```python
import jax
import jax.numpy as jnp
from jax import lax

D = 512
HID = 512
NODE_DEV = 320
EDGE_DEV = 2048
SLOT = 96
FAR_SLOT = 16
REACH = 2
NODES = 2560
EDGES = 16384
N_GRAPH = 8


def draw_send_list(key, part):
    random_scores = jax.random.randint(key, (N_GRAPH * N_GRAPH, NODE_DEV), 0, 1 << 16)
    distinct_scores = random_scores * NODE_DEV + jnp.arange(NODE_DEV, dtype=jnp.int32)[None, :]
    ranked = jnp.argsort(distinct_scores, axis=1, stable=True)[:, :SLOT]
    return ranked.reshape(N_GRAPH, N_GRAPH, SLOT).astype(jnp.int32)


def draw_receiver_ref(key, part):
    subkeys = jax.random.split(key, 5)
    total_edges = N_GRAPH * EDGE_DEV
    shard_index = jnp.arange(total_edges, dtype=jnp.int32) // EDGE_DEV
    position = jnp.arange(total_edges, dtype=jnp.int32) % EDGE_DEV
    category = jax.random.randint(subkeys[0], (total_edges,), 0, 10)
    local_node = jax.random.randint(subkeys[1], (total_edges,), 0, NODE_DEV)
    near_pick = jax.random.randint(subkeys[2], (total_edges,), 0, 2 * REACH)
    near_offset = jnp.where(near_pick < REACH, near_pick - REACH, near_pick - REACH + 1)
    far_offset = REACH + 1 + jax.random.randint(subkeys[3], (total_edges,), 0, N_GRAPH - 2 * REACH - 1)
    near_slot = jax.random.randint(subkeys[4], (total_edges,), 0, SLOT)
    far_slot = near_slot % FAR_SLOT
    near_offset = jnp.where(position == 1, 1, near_offset)
    near_slot = jnp.where(position == 1, SLOT - 1, near_slot)
    far_offset = jnp.where(position == 0, REACH + 1, far_offset)
    far_slot = jnp.where(position == 0, FAR_SLOT - 1, far_slot)
    category = jnp.where(position == 0, 0, jnp.where(position == 1, 1, category))
    near_value = NODE_DEV + (shard_index + near_offset) % N_GRAPH * SLOT + near_slot
    far_value = NODE_DEV + (shard_index + far_offset) % N_GRAPH * SLOT + far_slot
    return jnp.where(category == 0, far_value, jnp.where(category < 5, near_value, local_node)).astype(jnp.int32)


def draw_edge_count(key, part):
    count_key, full_key = jax.random.split(key)
    edge_totals = jax.random.randint(count_key, (N_GRAPH,), EDGE_DEV // 2, EDGE_DEV + 1)
    fullest = jax.random.randint(full_key, (), 0, N_GRAPH)
    return jnp.where(jnp.arange(N_GRAPH) == fullest, EDGE_DEV, edge_totals).astype(jnp.int32)


def place_ends(drawn, rng, low, largest):
    index_at = [jax.random.randint(jax.random.fold_in(rng, axis), (), 0, length) for axis, length in enumerate(drawn.shape)]
    main_axis = drawn.shape.index(max(drawn.shape))
    neighbour = index_at[:main_axis] + [(index_at[main_axis] + 1) % drawn.shape[main_axis]] + index_at[main_axis + 1:]
    return drawn.at[tuple(index_at)].set(low).at[tuple(neighbour)].set(largest)


def levels(stream_key, dims, cuts, low, high):
    loudness, own = 1.0, jax.random.fold_in(stream_key, 6)
    for dim, parts in cuts:
        steps = jnp.exp(jax.random.uniform(jax.random.fold_in(own, dim), (parts,), jnp.float32, low / len(cuts), high / len(cuts)))
        loudness = loudness * jnp.repeat(steps, dims[dim] // parts).reshape([-1 if axis == dim else 1 for axis in range(len(dims))])
    return loudness


def centred(stream_key, dims, width, reach, pieces=(), kind=jnp.bfloat16):
    entries = width * jax.random.normal(stream_key, dims, jnp.float32)
    if pieces:
        entries = entries * levels(stream_key, dims, pieces, -0.22, 0.18)
    return jnp.clip(entries, -reach, reach).astype(kind)


def setup_inputs(seed: int = 0) -> dict:
    splits = jax.random.split(jax.random.key(seed), 15)
    node_feats = centred(splits[0], (NODES, D), 1.0, 6.0, ((0, 32),))
    edge_feats = centred(splits[1], (EDGES, D), 1.0, 6.0, ((0, 32),))
    senders = place_ends(jax.random.randint(splits[2], (EDGES,), 0, NODE_DEV), jax.random.fold_in(splits[2], 1), 0, NODE_DEV - 1).astype(jnp.int32)
    receiver_ref = draw_receiver_ref(jax.random.fold_in(splits[14], 71), 0)
    send_list = draw_send_list(jax.random.fold_in(splits[14], 71), 0)
    edge_count = draw_edge_count(jax.random.fold_in(splits[14], 71), 0)
    edge_w1 = centred(splits[6], (3 * D, HID), (3 * D) ** -0.5, 0.15625)
    edge_w2 = centred(splits[7], (HID, D), HID ** -0.5, 0.25)
    edge_gain = jnp.clip(1.0 + 0.18 * jax.random.normal(splits[8], (D,), jnp.float32), 0.099609375, 1.8984375).astype(jnp.bfloat16)
    edge_shift = centred(splits[9], (D,), 0.5, 3.0)
    node_w1 = centred(splits[10], (2 * D, HID), (2 * D) ** -0.5, 0.1875)
    node_w2 = centred(splits[11], (HID, D), HID ** -0.5, 0.25)
    node_gain = jnp.clip(1.0 + 0.18 * jax.random.normal(splits[12], (D,), jnp.float32), 0.099609375, 1.8984375).astype(jnp.bfloat16)
    node_shift = centred(splits[13], (D,), 0.5, 3.0)
    return dict(node_feats=node_feats, edge_feats=edge_feats, senders=senders, receiver_ref=receiver_ref, send_list=send_list, edge_count=edge_count, edge_w1=edge_w1, edge_w2=edge_w2, edge_gain=edge_gain, edge_shift=edge_shift, node_w1=node_w1, node_w2=node_w2, node_gain=node_gain, node_shift=node_shift)


epsilon = 1e-05

def layer_norm(outputs, norm_gain, norm_shift):
    average = lax.optimization_barrier(jnp.mean(outputs, axis=-1, keepdims=True))
    centered = outputs - average
    variance = lax.optimization_barrier(jnp.mean(centered * centered, axis=-1, keepdims=True))
    return centered * lax.rsqrt(variance + epsilon) * norm_gain + norm_shift

def perceptron(inputs, first_weight, second_weight, norm_gain, norm_shift):
    joined = jnp.concatenate(inputs, axis=1)
    activation = jnp.dot(joined, first_weight, preferred_element_type=jnp.float32)
    hidden = jax.nn.silu(activation).astype(jnp.bfloat16)
    outputs = jnp.dot(hidden, second_weight, preferred_element_type=jnp.float32)
    return layer_norm(outputs, norm_gain, norm_shift)

def reference(node_feats, edge_feats, senders, receiver_ref, send_list, edge_count, edge_w1, edge_w2, edge_gain, edge_shift, node_w1, node_w2, node_gain, node_shift):
    positions = jnp.arange(EDGE_DEV, dtype=jnp.int32)

    def shard_step(aggregate, shard_index):
        first_edge = shard_index * EDGE_DEV
        edge_block = lax.dynamic_slice_in_dim(edge_feats, first_edge, EDGE_DEV, 0)
        sender_block = lax.dynamic_slice_in_dim(senders, first_edge, EDGE_DEV, 0)
        ref_block = lax.dynamic_slice_in_dim(receiver_ref, first_edge, EDGE_DEV, 0)
        offset = jnp.maximum(ref_block - NODE_DEV, 0)
        source = offset // SLOT
        slot_index = offset % SLOT
        column = lax.dynamic_index_in_dim(send_list, shard_index, 1, keepdims=False)
        remote = source * NODE_DEV + column[source, slot_index]
        receivers = jnp.where(ref_block < NODE_DEV, shard_index * NODE_DEV + ref_block, remote).astype(jnp.int32)
        sender_rows = node_feats[(shard_index * NODE_DEV + sender_block).astype(jnp.int32)]
        receiver_rows = node_feats[receivers]
        update = edge_block.astype(jnp.float32) + perceptron((edge_block, sender_rows, receiver_rows), edge_w1, edge_w2, edge_gain, edge_shift)
        live_mask = positions < edge_count[shard_index]
        new_rows = jnp.where(live_mask[:, None], update, edge_block.astype(jnp.float32)).astype(jnp.bfloat16)
        messages = jnp.where(live_mask[:, None], new_rows.astype(jnp.float32), 0.0)
        aggregate = aggregate.at[receivers].add(messages)
        return (aggregate, new_rows)
    aggregate, new_edges = lax.scan(shard_step, jnp.zeros((NODES, D), jnp.float32), jnp.arange(N_GRAPH, dtype=jnp.int32))
    new_edges = new_edges.reshape(EDGES, D)
    node_update = node_feats.astype(jnp.float32) + perceptron((node_feats, aggregate.astype(jnp.bfloat16)), node_w1, node_w2, node_gain, node_shift)
    return (new_edges, node_update.astype(jnp.bfloat16))
```

```python
import functools

import jax
import jax.numpy as jnp
from jax import lax
from jax.experimental import pallas as pl
from jax.experimental.pallas import tpu as pltpu
from jax.sharding import PartitionSpec as P

FAR_SLOT = 16
REACH = 2
EPSILON = 1e-05
MESH = pl.DeviceIdType.MESH
F32 = jnp.float32
BF16 = jnp.bfloat16


def dot(a, b):
    return jnp.dot(a, b, preferred_element_type=F32)


def iota(shape, dim):
    return lax.broadcasted_iota(jnp.int32, shape, dim)


def silu(v):
    half = 0.5 * v
    return half + half * jnp.tanh(half)


def layer_norm(y, gain, shift):
    width = y.shape[1]
    mean = jnp.sum(y, axis=1, keepdims=True) * (1.0 / width)
    c = y - mean
    var = jnp.sum(c * c, axis=1, keepdims=True) * (1.0 / width)
    return c * lax.rsqrt(var + EPSILON) * gain + shift


def kernel(
    groups, feats,
    count_ref, nf, send_ref, recv_ref, list_ref, eg, es, ng, ns,
    ef_hbm, w1_hbm, w2_hbm, n1_hbm, n2_hbm,
    new_edges_hbm, new_nodes_hbm,
    ef, w1, w2, n1, n2, tab, lst, part, pair, halo, ret, agg_out, cross, agg, pre, oute, outn,
    load_sem, store_sem,
    ag_s, ag_r, rel_s, rel_r, h_s, h_r, hr_s, hr_r, p_s, p_r, b_s, b_r, x_s, x_r, d_s, d_r,
):
    g = lax.axis_index("graph")
    f = lax.axis_index("feat")
    n_own = nf.shape[0]
    width = nf.shape[1]
    half = width // 2
    edges = ef_hbm.shape[0]
    slot = list_ref.shape[2]
    region = n_own * feats
    chips = feats // 2
    chip = f // 2
    h = lax.rem(f, 2)
    other = 1 - h
    partner = chip * 2 + other
    mine = pl.ds(pl.multiple_of(h * half, half), half)
    theirs = pl.ds(pl.multiple_of(other * half, half), half)
    near = [d for d in range(1, REACH + 1)] + [groups - d for d in range(REACH, 0, -1)]
    far = list(range(REACH + 1, groups - REACH))
    blocks = [(d, i * slot, slot) for i, d in enumerate(near)]
    blocks += [(d, len(near) * slot + i * FAR_SLOT, FAR_SLOT) for i, d in enumerate(far)]
    order = list(range(len(near), len(blocks))) + [1, 2, 0, 3]
    listed = len(near) * slot + len(far) * FAR_SLOT

    def to(graph, feat):
        return {"graph": graph, "feat": feat}

    barrier = pltpu.get_barrier_semaphore()
    for k in range(1, feats):
        pl.semaphore_signal(barrier, inc=1, device_id=to(g, lax.rem(f + k, feats)), device_id_type=MESH)
    for d in range(1, groups):
        pl.semaphore_signal(barrier, inc=1, device_id=to(lax.rem(g + d, groups), f), device_id_type=MESH)

    loads = [
        pltpu.make_async_copy(src, dst, load_sem.at[i])
        for i, (src, dst) in enumerate(((ef_hbm, ef), (w1_hbm, w1), (w2_hbm, w2), (n1_hbm, n1), (n2_hbm, n2)))
    ]
    for load in loads:
        load.start()

    own_rows = pl.ds(pl.multiple_of(f * n_own, n_own), n_own)
    tab[own_rows, :] = nf[...]

    rr = recv_ref[...]
    offset = jnp.maximum(rr - region, 0)
    source = jnp.floor((offset.astype(F32) + 0.5) * (1.0 / slot)).astype(jnp.int32)
    slot_index = offset - source * slot
    dist = source - g
    dist = jnp.where(dist < 0, dist + groups, dist)
    base = len(near) * slot + (dist - REACH - 1) * FAR_SLOT
    for i, d in enumerate(near):
        base = jnp.where(dist == d, i * slot, base)
    row_index = jnp.where(rr < region, rr, region + base + slot_index)
    count = count_ref[0]
    live_lane = f * edges + iota((1, edges), 1) < count
    row_index = jnp.where(live_lane, row_index, -1)

    def down(index):
        wide = jnp.broadcast_to(index.astype(F32), (128, edges))
        return wide.T.astype(jnp.int32)

    def select(column, first, many):
        pieces = []
        for k in range(0, many, 128):
            w = min(128, many - k)
            pieces.append((column == iota((edges, 128), 1) + (first + k)).astype(F32).astype(BF16)[:, :w])
        return jnp.concatenate(pieces, axis=1) if len(pieces) > 1 else pieces[0]

    def list_rows(d, rows):
        index = list_ref[0, pl.ds(lax.rem(g + groups - d, groups), 1), :]
        return (iota((region, slot), 0) == index).astype(F32)[:, :rows]

    pl.semaphore_wait(barrier, feats - 1 + groups - 1)

    own_copy = pltpu.make_async_remote_copy(
        nf, tab.at[own_rows, :], ag_s.at[0], ag_r.at[0], device_id=to(g, partner), device_id_type=MESH)
    chip_copies = []
    for j in range(1, chips):
        for rel in range(2):
            hh = h if rel == 0 else other
            cols = mine if rel == 0 else theirs
            k = 1 + (j - 1) * 2 + rel
            chip_copies.append(pltpu.make_async_remote_copy(
                nf.at[:, cols], tab.at[own_rows, cols], ag_s.at[k], ag_r.at[k],
                device_id=to(g, lax.rem(chip + j, chips) * 2 + hh), device_id_type=MESH))
    for c in chip_copies:
        c.start()
    own_copy.start()

    loads[0].wait()
    loads[1].wait()
    pre[...] = dot(ef[...], w1[0:width, :])

    for c in chip_copies:
        c.wait_recv()
    own_copy.wait_recv()
    relays = []
    for j in range(1, chips):
        at = tab.at[pl.ds(pl.multiple_of(lax.rem(chip + chips - j, chips) * 2 * n_own, 2 * n_own), 2 * n_own), mine]
        relays.append(pltpu.make_async_remote_copy(
            at, at, rel_s.at[j - 1], rel_r.at[j - 1], device_id=to(g, partner), device_id_type=MESH))

    nodes_half = tab[0:region, mine]
    for i, (d, first, rows) in enumerate(blocks):
        lst[first:first + rows, :] = lax.dot_general(
            list_rows(d, rows).astype(BF16), nodes_half, (((0,), (0,)), ((), ())),
            preferred_element_type=F32).astype(BF16)
    halo_copies = {}
    for i in order:
        d, first, rows = blocks[i]
        halo_copies[i] = pltpu.make_async_remote_copy(
            lst.at[first:first + rows, :], halo.at[first:first + rows, mine], h_s.at[i], h_r.at[i],
            device_id=to(lax.rem(g + groups - d, groups), f), device_id_type=MESH)
        halo_copies[i].start()
    for c in relays:
        c.start()
    for c in relays:
        c.wait_recv()

    sender_sel = select(down(send_ref[...]), 0, region)
    column = down(row_index)
    pre[...] += dot(dot(sender_sel, tab[0:region, :]).astype(BF16), w1[width:2 * width, :])
    local_rows = dot(select(column, 0, region), tab[0:region, :]).astype(BF16)
    pre[...] += dot(local_rows, w1[2 * width:3 * width, :])

    share = {}
    for i in order:
        d, first, rows = blocks[i]
        halo_copies[i].wait_recv()
        at = halo.at[first:first + rows, mine]
        share[i] = pltpu.make_async_remote_copy(
            at, at, hr_s.at[i], hr_r.at[i], device_id=to(g, partner), device_id_type=MESH)
        share[i].start()
    for i in order:
        share[i].wait_recv()

    loads[2].wait()
    halo_sel = select(column, region, listed)
    table = halo[...]
    gain, shift = eg[...].astype(F32), es[...].astype(F32)
    step = edges // 2
    for k in range(0, edges, step):
        rows = slice(k, k + step)
        v = pre[rows, :] + dot(dot(halo_sel[rows, :], table).astype(BF16), w1[2 * width:3 * width, :])
        y = dot(silu(v).astype(BF16), w2[...])
        feats_in = ef[rows, :].astype(F32)
        update = feats_in + layer_norm(y, gain, shift)
        live = f * edges + k + iota((step, 1), 0) < count
        oute[rows, :] = jnp.where(live, update, feats_in).astype(BF16)

    edge_store = pltpu.make_async_copy(oute, new_edges_hbm, store_sem.at[0])
    edge_store.start()

    messages = oute[...]
    halo_selT = (iota((listed, edges), 0) + region == row_index).astype(F32).astype(BF16)
    part[0:listed, :] = dot(halo_selT, messages)
    pair_out = agg_out
    pair_out[0:listed, :] = part[0:listed, theirs].astype(BF16)
    first_pair = pltpu.make_async_remote_copy(
        pair_out.at[0:listed, :], pair.at[0:listed, :], p_s.at[0], p_r.at[0],
        device_id=to(g, partner), device_id_type=MESH)
    first_pair.start()
    own_selT = (iota((region, edges), 0) == row_index).astype(F32).astype(BF16)
    part[listed:listed + region, :] = dot(own_selT, messages)
    pair_out[listed:listed + region, :] = part[listed:listed + region, theirs].astype(BF16)
    second_pair = pltpu.make_async_remote_copy(
        pair_out.at[listed:listed + region, :], pair.at[listed:listed + region, :], p_s.at[1], p_r.at[1],
        device_id=to(g, partner), device_id_type=MESH)
    second_pair.start()

    first_pair.wait_recv()
    for c in halo_copies.values():
        c.wait_send()
    lst[...] = (part[0:listed, mine] + pair[0:listed, :].astype(F32)).astype(BF16)
    back = {}
    for i in order:
        d, first, rows = blocks[i]
        back[i] = pltpu.make_async_remote_copy(
            lst.at[first:first + rows, :], ret.at[first:first + rows, :], b_s.at[i], b_r.at[i],
            device_id=to(lax.rem(g + d, groups), f), device_id_type=MESH)
        back[i].start()

    loads[3].wait()
    loads[4].wait()
    node_in = nf[...]
    node_pre = dot(node_in, n1[0:width, :])
    second_pair.wait_recv()
    total = part[listed:listed + region, mine] + pair[listed:listed + region, :].astype(F32)
    for i in order:
        d, first, rows = blocks[i]
        back[i].wait_recv()
        total += dot(list_rows(d, rows).astype(BF16), ret[first:first + rows, :])
    part[0:region, 0:half] = total

    chip_rows = 2 * n_own
    for j in range(1, chips):
        at = pl.ds(pl.multiple_of(lax.rem(chip + j, chips) * chip_rows, chip_rows), chip_rows)
        cross[0, j - 1] = part[at, 0:half].astype(BF16)
    crosses = []
    for j in range(1, chips):
        crosses.append(pltpu.make_async_remote_copy(
            cross.at[0, j - 1], cross.at[1, j - 1], x_s.at[j - 1], x_r.at[j - 1],
            device_id=to(g, lax.rem(chip + j, chips) * 2 + h), device_id_type=MESH))
        crosses[-1].start()

    def chip_total(which):
        at = pl.ds(pl.multiple_of((chip * 2 + which) * n_own, n_own), n_own)
        rows = part[at, 0:half]
        local = pl.ds(pl.multiple_of(which * n_own, n_own), n_own)
        for j in range(1, chips):
            rows = rows + cross[1, j - 1, local, :].astype(F32)
        return rows.astype(BF16)

    for c in crosses:
        c.wait_recv()
    agg[0, :, 0:half] = chip_total(other)
    last = pltpu.make_async_remote_copy(
        agg.at[0, :, 0:half], agg.at[1, :, mine], d_s.at[0], d_r.at[0],
        device_id=to(g, partner), device_id_type=MESH)
    last.start()
    agg[1, :, mine] = chip_total(h)
    last.wait_recv()
    node_pre = node_pre + dot(agg[1], n1[width:2 * width, :])
    node_out = dot(silu(node_pre).astype(BF16), n2[...])
    outn[...] = (node_in.astype(F32) + layer_norm(node_out, ng[...].astype(F32), ns[...].astype(F32))).astype(BF16)
    node_store = pltpu.make_async_copy(outn, new_nodes_hbm, store_sem.at[1])
    node_store.start()

    own_copy.wait_send()
    for c in chip_copies + relays + list(share.values()) + [first_pair, second_pair]:
        c.wait_send()
    for c in list(back.values()) + crosses + [last]:
        c.wait_send()
    edge_store.wait()
    node_store.wait()


def per_device(node_feats, edge_feats, senders, receiver_ref, send_list, edge_count,
               edge_w1, edge_w2, edge_gain, edge_shift, node_w1, node_w2, node_gain, node_shift):
    groups = lax.axis_size("graph")
    feats = lax.axis_size("feat")
    n_own, width = node_feats.shape
    edges = edge_feats.shape[0]
    slot = send_list.shape[2]
    half = width // 2
    region = n_own * feats
    blocks = groups - 1
    listed = 2 * REACH * slot + (groups - 1 - 2 * REACH) * FAR_SLOT
    chips = feats // 2
    vmem = pl.BlockSpec(memory_space=pltpu.VMEM)
    hbm = pl.BlockSpec(memory_space=pl.ANY)
    smem = pl.BlockSpec(memory_space=pltpu.SMEM)
    dma = lambda n: pltpu.SemaphoreType.DMA((n,))
    links = 2 * max(chips - 1, 0) + 1
    return pl.pallas_call(
        functools.partial(kernel, groups, feats),
        out_shape=(jax.ShapeDtypeStruct((edges, width), BF16), jax.ShapeDtypeStruct((n_own, width), BF16)),
        in_specs=[smem] + [vmem] * 8 + [hbm] * 5,
        out_specs=(hbm, hbm),
        scratch_shapes=[
            pltpu.VMEM(edge_feats.shape, BF16), pltpu.VMEM(edge_w1.shape, BF16), pltpu.VMEM(edge_w2.shape, BF16),
            pltpu.VMEM(node_w1.shape, BF16), pltpu.VMEM(node_w2.shape, BF16),
            pltpu.VMEM((region, width), BF16),
            pltpu.VMEM((listed, half), BF16),
            pltpu.VMEM((listed + region, width), F32),
            pltpu.VMEM((listed + region, half), BF16),
            pltpu.VMEM((listed, width), BF16),
            pltpu.VMEM((listed, half), BF16),
            pltpu.VMEM((listed + region, half), BF16),
            pltpu.VMEM((2, chips - 1, 2 * n_own, half), BF16),
            pltpu.VMEM((2, n_own, width), BF16),
            pltpu.VMEM((edges, edge_w1.shape[1]), F32),
            pltpu.VMEM((edges, width), BF16),
            pltpu.VMEM((n_own, width), BF16),
            dma(5), dma(2),
            dma(links), dma(links), dma(chips - 1), dma(chips - 1),
            dma(blocks), dma(blocks), dma(blocks), dma(blocks),
            dma(2), dma(2), dma(blocks), dma(blocks), dma(chips - 1), dma(chips - 1), dma(1), dma(1),
        ],
        compiler_params=pltpu.CompilerParams(
            collective_id=0, has_side_effects=True, vmem_limit_bytes=60 * 1024 * 1024),
    )(edge_count, node_feats, senders.reshape(1, edges), receiver_ref.reshape(1, edges), send_list,
      edge_gain.reshape(1, width), edge_shift.reshape(1, width),
      node_gain.reshape(1, width), node_shift.reshape(1, width),
      edge_feats, edge_w1, edge_w2, node_w1, node_w2)


def solution(mesh):
    whole = P()
    rows = P(("graph", "feat"), None)
    flat = P(("graph", "feat"))
    return jax.shard_map(
        per_device,
        mesh=mesh,
        in_specs=(rows, rows, flat, flat, P("graph", None, None), P("graph")) + (whole,) * 8,
        out_specs=(rows, rows),
        check_vma=False,
    )
```

```python
import functools

import jax
import jax.numpy as jnp
from jax import lax
from jax.experimental import pallas as pl
from jax.experimental.pallas import tpu as pltpu
from jax.sharding import PartitionSpec as P

FAR_SLOT = 16
REACH = 2
EPSILON = 1e-05
MESH = pl.DeviceIdType.MESH
F32 = jnp.float32
BF16 = jnp.bfloat16


def dot(a, b):
    return jnp.dot(a, b, preferred_element_type=F32)


def iota(shape, dim):
    return lax.broadcasted_iota(jnp.int32, shape, dim)


def silu(v):
    half = 0.5 * v
    return half + half * jnp.tanh(half)


def layer_norm(y, gain, shift):
    width = y.shape[1]
    mean = jnp.sum(y, axis=1, keepdims=True) * (1.0 / width)
    c = y - mean
    var = jnp.sum(c * c, axis=1, keepdims=True) * (1.0 / width)
    return c * lax.rsqrt(var + EPSILON) * gain + shift


def kernel(
    groups, feats,
    count_hbm, nf_hbm, send_hbm, recv_hbm, list_hbm, eg_hbm, es_hbm, ng_hbm, ns_hbm,
    ef_hbm, w1_hbm, w2_hbm, n1_hbm, n2_hbm,
    oute, outn,
    count_ref, nf, send_ref, recv_ref, list_ref, eg, es, ng, ns,
    ef, w1, w2, n1, n2, tab, lst, part, pair, halo, ret, agg_out, cross, agg, pre,
    load_sem,
    ag_s, ag_r, rel_s, rel_r, h_s, h_r, hr_s, hr_r, p_s, p_r, b_s, b_r, x_s, x_r, d_s, d_r,
):
    g = lax.axis_index("graph")
    f = lax.axis_index("feat")
    n_own, width = nf.shape
    half = width // 2
    edges = ef_hbm.shape[0]
    slot = list_hbm.shape[2]
    region = n_own * feats
    chips = feats // 2
    chip = f // 2
    h = lax.rem(f, 2)
    other = 1 - h
    partner = chip * 2 + other
    mine = pl.ds(pl.multiple_of(h * half, half), half)
    theirs = pl.ds(pl.multiple_of(other * half, half), half)
    near = [d for d in range(1, REACH + 1)] + [groups - d for d in range(REACH, 0, -1)]
    far = list(range(REACH + 1, groups - REACH))
    blocks = [(d, i * slot, slot) for i, d in enumerate(near)]
    blocks += [(d, len(near) * slot + i * FAR_SLOT, FAR_SLOT) for i, d in enumerate(far)]
    order = list(range(len(near), len(blocks))) + [1, 2, 0, 3]
    listed = len(near) * slot + len(far) * FAR_SLOT

    def to(graph, feat):
        return {"graph": graph, "feat": feat}

    barrier = pltpu.get_barrier_semaphore()
    for k in range(1, feats):
        pl.semaphore_signal(barrier, inc=1, device_id=to(g, lax.rem(f + k, feats)), device_id_type=MESH)
    for d in range(1, groups):
        pl.semaphore_signal(barrier, inc=1, device_id=to(lax.rem(g + d, groups), f), device_id_type=MESH)

    loads = [
        pltpu.make_async_copy(src, dst, load_sem.at[i])
        for i, (src, dst) in enumerate((
            (nf_hbm, nf), (recv_hbm, recv_ref), (send_hbm, send_ref), (count_hbm, count_ref), (list_hbm, list_ref),
            (ef_hbm, ef), (w1_hbm, w1), (w2_hbm, w2), (eg_hbm, eg), (es_hbm, es),
            (n1_hbm, n1), (n2_hbm, n2), (ng_hbm, ng), (ns_hbm, ns)))
    ]
    for load in loads:
        load.start()
    for load in loads[:5]:
        load.wait()

    own_rows = pl.ds(pl.multiple_of(f * n_own, n_own), n_own)
    tab[own_rows, :] = nf[...]

    rr = recv_ref[...]
    offset = jnp.maximum(rr - region, 0)
    source = jnp.floor((offset.astype(F32) + 0.5) * (1.0 / slot)).astype(jnp.int32)
    slot_index = offset - source * slot
    dist = source - g
    dist = jnp.where(dist < 0, dist + groups, dist)
    base = len(near) * slot + (dist - REACH - 1) * FAR_SLOT
    for i, d in enumerate(near):
        base = jnp.where(dist == d, i * slot, base)
    row_index = jnp.where(rr < region, rr, region + base + slot_index)
    count = count_ref[0]
    live_lane = f * edges + iota((1, edges), 1) < count
    row_index = jnp.where(live_lane, row_index, -1)

    def down(index):
        wide = jnp.broadcast_to(index.astype(F32), (128, edges))
        return wide.T.astype(jnp.int32)

    def select(column, first, many):
        pieces = []
        for k in range(0, many, 128):
            w = min(128, many - k)
            pieces.append((column == iota((edges, 128), 1) + (first + k)).astype(F32).astype(BF16)[:, :w])
        return jnp.concatenate(pieces, axis=1) if len(pieces) > 1 else pieces[0]

    def list_rows(d, rows):
        index = list_ref[0, pl.ds(lax.rem(g + groups - d, groups), 1), :]
        return (iota((region, slot), 0) == index).astype(F32)[:, :rows]

    pl.semaphore_wait(barrier, feats - 1 + groups - 1)

    own_copy = pltpu.make_async_remote_copy(
        nf, tab.at[own_rows, :], ag_s.at[0], ag_r.at[0], device_id=to(g, partner), device_id_type=MESH)
    chip_copies = []
    for j in range(1, chips):
        for rel in range(2):
            hh = h if rel == 0 else other
            cols = mine if rel == 0 else theirs
            k = 1 + (j - 1) * 2 + rel
            chip_copies.append(pltpu.make_async_remote_copy(
                nf.at[:, cols], tab.at[own_rows, cols], ag_s.at[k], ag_r.at[k],
                device_id=to(g, lax.rem(chip + j, chips) * 2 + hh), device_id_type=MESH))
    for c in chip_copies:
        c.start()
    own_copy.start()

    loads[5].wait()
    loads[6].wait()
    pre[...] = dot(ef[...], w1[0:width, :])

    for c in chip_copies:
        c.wait_recv()
    own_copy.wait_recv()
    relays = []
    for j in range(1, chips):
        at = tab.at[pl.ds(pl.multiple_of(lax.rem(chip + chips - j, chips) * 2 * n_own, 2 * n_own), 2 * n_own), mine]
        relays.append(pltpu.make_async_remote_copy(
            at, at, rel_s.at[j - 1], rel_r.at[j - 1], device_id=to(g, partner), device_id_type=MESH))

    nodes_half = tab[0:region, mine]
    for i, (d, first, rows) in enumerate(blocks):
        lst[first:first + rows, :] = lax.dot_general(
            list_rows(d, rows).astype(BF16), nodes_half, (((0,), (0,)), ((), ())),
            preferred_element_type=F32).astype(BF16)
    halo_copies = {}
    for i in order:
        d, first, rows = blocks[i]
        halo_copies[i] = pltpu.make_async_remote_copy(
            lst.at[first:first + rows, :], halo.at[first:first + rows, mine], h_s.at[i], h_r.at[i],
            device_id=to(lax.rem(g + groups - d, groups), f), device_id_type=MESH)
        halo_copies[i].start()
    for c in relays:
        c.start()
    for c in relays:
        c.wait_recv()

    sender_sel = select(down(send_ref[...]), 0, region)
    column = down(row_index)
    pre[...] += dot(dot(sender_sel, tab[0:region, :]).astype(BF16), w1[width:2 * width, :])
    local_rows = dot(select(column, 0, region), tab[0:region, :]).astype(BF16)
    pre[...] += dot(local_rows, w1[2 * width:3 * width, :])

    share = {}
    for i in order:
        d, first, rows = blocks[i]
        halo_copies[i].wait_recv()
        at = halo.at[first:first + rows, mine]
        share[i] = pltpu.make_async_remote_copy(
            at, at, hr_s.at[i], hr_r.at[i], device_id=to(g, partner), device_id_type=MESH)
        share[i].start()
    for i in order:
        share[i].wait_recv()

    for load in loads[7:10]:
        load.wait()
    halo_sel = select(column, region, listed)
    table = halo[...]
    gain, shift = eg[...].astype(F32).reshape(1, width), es[...].astype(F32).reshape(1, width)
    step = edges // 2
    for k in range(0, edges, step):
        rows = slice(k, k + step)
        v = pre[rows, :] + dot(dot(halo_sel[rows, :], table).astype(BF16), w1[2 * width:3 * width, :])
        y = dot(silu(v).astype(BF16), w2[...])
        feats_in = ef[rows, :].astype(F32)
        update = feats_in + layer_norm(y, gain, shift)
        live = f * edges + k + iota((step, 1), 0) < count
        oute[rows, :] = jnp.where(live, update, feats_in).astype(BF16)

    messages = oute[...]
    halo_selT = (iota((listed, edges), 0) + region == row_index).astype(F32).astype(BF16)
    part[0:listed, :] = dot(halo_selT, messages)
    pair_out = agg_out
    pair_out[0:listed, :] = part[0:listed, theirs].astype(BF16)
    first_pair = pltpu.make_async_remote_copy(
        pair_out.at[0:listed, :], pair.at[0:listed, :], p_s.at[0], p_r.at[0],
        device_id=to(g, partner), device_id_type=MESH)
    first_pair.start()
    own_selT = (iota((region, edges), 0) == row_index).astype(F32).astype(BF16)
    part[listed:listed + region, :] = dot(own_selT, messages)
    pair_out[listed:listed + region, :] = part[listed:listed + region, theirs].astype(BF16)
    second_pair = pltpu.make_async_remote_copy(
        pair_out.at[listed:listed + region, :], pair.at[listed:listed + region, :], p_s.at[1], p_r.at[1],
        device_id=to(g, partner), device_id_type=MESH)
    second_pair.start()

    first_pair.wait_recv()
    for c in halo_copies.values():
        c.wait_send()
    lst[...] = (part[0:listed, mine] + pair[0:listed, :].astype(F32)).astype(BF16)
    back = {}
    for i in order:
        d, first, rows = blocks[i]
        back[i] = pltpu.make_async_remote_copy(
            lst.at[first:first + rows, :], ret.at[first:first + rows, :], b_s.at[i], b_r.at[i],
            device_id=to(lax.rem(g + d, groups), f), device_id_type=MESH)
        back[i].start()

    for load in loads[10:14]:
        load.wait()
    node_in = nf[...]
    node_pre = dot(node_in, n1[0:width, :])
    second_pair.wait_recv()
    total = part[listed:listed + region, mine] + pair[listed:listed + region, :].astype(F32)
    for i in order:
        d, first, rows = blocks[i]
        back[i].wait_recv()
        total += dot(list_rows(d, rows).astype(BF16), ret[first:first + rows, :])
    part[0:region, 0:half] = total

    chip_rows = 2 * n_own
    for j in range(1, chips):
        at = pl.ds(pl.multiple_of(lax.rem(chip + j, chips) * chip_rows, chip_rows), chip_rows)
        cross[0, j - 1] = part[at, 0:half].astype(BF16)
    crosses = []
    for j in range(1, chips):
        crosses.append(pltpu.make_async_remote_copy(
            cross.at[0, j - 1], cross.at[1, j - 1], x_s.at[j - 1], x_r.at[j - 1],
            device_id=to(g, lax.rem(chip + j, chips) * 2 + h), device_id_type=MESH))
        crosses[-1].start()

    def chip_total(which):
        at = pl.ds(pl.multiple_of((chip * 2 + which) * n_own, n_own), n_own)
        rows = part[at, 0:half]
        local = pl.ds(pl.multiple_of(which * n_own, n_own), n_own)
        for j in range(1, chips):
            rows = rows + cross[1, j - 1, local, :].astype(F32)
        return rows.astype(BF16)

    for c in crosses:
        c.wait_recv()
    agg[0, :, 0:half] = chip_total(other)
    last = pltpu.make_async_remote_copy(
        agg.at[0, :, 0:half], agg.at[1, :, mine], d_s.at[0], d_r.at[0],
        device_id=to(g, partner), device_id_type=MESH)
    last.start()
    agg[1, :, mine] = chip_total(h)
    last.wait_recv()
    node_pre = node_pre + dot(agg[1], n1[width:2 * width, :])
    node_out = dot(silu(node_pre).astype(BF16), n2[...])
    outn[...] = (node_in.astype(F32) + layer_norm(node_out, ng[...].astype(F32).reshape(1, width), ns[...].astype(F32).reshape(1, width))).astype(BF16)

    own_copy.wait_send()
    for c in chip_copies + relays + list(share.values()) + [first_pair, second_pair]:
        c.wait_send()
    for c in list(back.values()) + crosses + [last]:
        c.wait_send()


def per_device(node_feats, edge_feats, senders, receiver_ref, send_list, edge_count,
               edge_w1, edge_w2, edge_gain, edge_shift, node_w1, node_w2, node_gain, node_shift):
    groups = lax.axis_size("graph")
    feats = lax.axis_size("feat")
    n_own, width = node_feats.shape
    edges = edge_feats.shape[0]
    slot = send_list.shape[2]
    half = width // 2
    region = n_own * feats
    blocks = groups - 1
    listed = 2 * REACH * slot + (groups - 1 - 2 * REACH) * FAR_SLOT
    chips = feats // 2
    vmem = pl.BlockSpec(memory_space=pltpu.VMEM)
    hbm = pl.BlockSpec(memory_space=pl.ANY)
    dma = lambda n: pltpu.SemaphoreType.DMA((n,))
    links = 2 * max(chips - 1, 0) + 1
    return pl.pallas_call(
        functools.partial(kernel, groups, feats),
        out_shape=(pltpu.VMEM((edges, width), BF16), pltpu.VMEM((n_own, width), BF16)),
        in_specs=[hbm] * 14,
        out_specs=(vmem, vmem),
        scratch_shapes=[
            pltpu.SMEM(edge_count.shape, jnp.int32), pltpu.VMEM(node_feats.shape, BF16),
            pltpu.VMEM((1, edges), jnp.int32), pltpu.VMEM((1, edges), jnp.int32), pltpu.VMEM(send_list.shape, jnp.int32),
        ] + [pltpu.VMEM((width,), BF16)] * 4 + [
            pltpu.VMEM(edge_feats.shape, BF16), pltpu.VMEM(edge_w1.shape, BF16), pltpu.VMEM(edge_w2.shape, BF16),
            pltpu.VMEM(node_w1.shape, BF16), pltpu.VMEM(node_w2.shape, BF16),
            pltpu.VMEM((region, width), BF16),
            pltpu.VMEM((listed, half), BF16),
            pltpu.VMEM((listed + region, width), F32),
            pltpu.VMEM((listed + region, half), BF16),
            pltpu.VMEM((listed, width), BF16),
            pltpu.VMEM((listed, half), BF16),
            pltpu.VMEM((listed + region, half), BF16),
            pltpu.VMEM((2, chips - 1, 2 * n_own, half), BF16),
            pltpu.VMEM((2, n_own, width), BF16),
            pltpu.VMEM((edges, edge_w1.shape[1]), F32),
            dma(14),
            dma(links), dma(links), dma(chips - 1), dma(chips - 1),
            dma(blocks), dma(blocks), dma(blocks), dma(blocks),
            dma(2), dma(2), dma(blocks), dma(blocks), dma(chips - 1), dma(chips - 1), dma(1), dma(1),
        ],
        compiler_params=pltpu.CompilerParams(
            collective_id=0, has_side_effects=True, vmem_limit_bytes=60 * 1024 * 1024),
    )(edge_count, node_feats, senders.reshape(1, edges), receiver_ref.reshape(1, edges), send_list,
      edge_gain, edge_shift, node_gain, node_shift,
      edge_feats, edge_w1, edge_w2, node_w1, node_w2)


def solution(mesh):
    whole = P()
    rows = P(("graph", "feat"), None)
    flat = P(("graph", "feat"))
    return jax.shard_map(
        per_device,
        mesh=mesh,
        in_specs=(rows, rows, flat, flat, P("graph", None, None), P("graph")) + (whole,) * 8,
        out_specs=(rows, rows),
        check_vma=False,
    )
```

```python
import functools

import jax
import jax.numpy as jnp
from jax import lax
from jax.experimental import pallas as pl
from jax.experimental.pallas import tpu as pltpu
from jax.sharding import PartitionSpec as P

FAR_SLOT = 16
REACH = 2
EPSILON = 1e-05
MESH = pl.DeviceIdType.MESH
F32 = jnp.float32
BF16 = jnp.bfloat16


def dot(a, b):
    return jnp.dot(a, b, preferred_element_type=F32)


def iota(shape, dim):
    return lax.broadcasted_iota(jnp.int32, shape, dim)


def silu(v):
    half = 0.5 * v
    return half + half * jnp.tanh(half)


def layer_norm(y, gain, shift):
    width = y.shape[1]
    mean = jnp.sum(y, axis=1, keepdims=True) * (1.0 / width)
    c = y - mean
    var = jnp.sum(c * c, axis=1, keepdims=True) * (1.0 / width)
    return c * lax.rsqrt(var + EPSILON) * gain + shift


def kernel(
    groups, feats,
    count_hbm, nf_hbm, send_hbm, recv_hbm, list_hbm, eg_hbm, es_hbm, ng_hbm, ns_hbm,
    ef_hbm, w1_hbm, w2_hbm, n1_hbm, n2_hbm,
    oute, outn,
    count_ref, nf, send_ref, recv_ref, list_ref, eg, es, ng, ns,
    ef, w1, w2, n1, n2, tab, lst, part, pair, halo, ret, pair_out, own16, sums, pre,
    list_sel, list_selT, recv_sel, recv_selT,
    load_sem,
    ag_s, ag_r, rel_s, rel_r, h_s, h_r, hr_s, hr_r, p_s, p_r, b_s, b_r, x_s, x_r,
):
    g = lax.axis_index("graph")
    f = lax.axis_index("feat")
    n_own, width = nf.shape
    half = width // 2
    edges = ef_hbm.shape[0]
    slot = list_hbm.shape[2]
    region = n_own * feats
    chips = feats // 2
    chip = f // 2
    h = lax.rem(f, 2)
    other = 1 - h
    partner = chip * 2 + other
    mine = pl.ds(pl.multiple_of(h * half, half), half)
    theirs = pl.ds(pl.multiple_of(other * half, half), half)
    near = [d for d in range(1, REACH + 1)] + [groups - d for d in range(REACH, 0, -1)]
    far = list(range(REACH + 1, groups - REACH))
    blocks = [(d, i * slot, slot) for i, d in enumerate(near)]
    blocks += [(d, len(near) * slot + i * FAR_SLOT, FAR_SLOT) for i, d in enumerate(far)]
    order = list(range(len(near), len(blocks))) + [1, 2, 0, 3]
    listed = len(near) * slot + len(far) * FAR_SLOT

    def to(graph, feat):
        return {"graph": graph, "feat": feat}

    barrier = pltpu.get_barrier_semaphore()
    for k in range(1, feats):
        pl.semaphore_signal(barrier, inc=1, device_id=to(g, lax.rem(f + k, feats)), device_id_type=MESH)
    for d in range(1, groups):
        pl.semaphore_signal(barrier, inc=1, device_id=to(lax.rem(g + d, groups), f), device_id_type=MESH)

    loads = [
        pltpu.make_async_copy(src, dst, load_sem.at[i])
        for i, (src, dst) in enumerate((
            (nf_hbm, nf), (recv_hbm, recv_ref), (send_hbm, send_ref), (count_hbm, count_ref), (list_hbm, list_ref),
            (ef_hbm, ef), (w1_hbm, w1), (w2_hbm, w2), (eg_hbm, eg), (es_hbm, es),
            (n1_hbm, n1), (n2_hbm, n2), (ng_hbm, ng), (ns_hbm, ns)))
    ]
    for load in loads:
        load.start()
    for load in loads[:5]:
        load.wait()

    own_rows = pl.ds(pl.multiple_of(f * n_own, n_own), n_own)
    tab[own_rows, :] = nf[...]

    rr = recv_ref[...]
    offset = jnp.maximum(rr - region, 0)
    source = jnp.floor((offset.astype(F32) + 0.5) * (1.0 / slot)).astype(jnp.int32)
    slot_index = offset - source * slot
    dist = source - g
    dist = jnp.where(dist < 0, dist + groups, dist)
    base = len(near) * slot + (dist - REACH - 1) * FAR_SLOT
    for i, d in enumerate(near):
        base = jnp.where(dist == d, i * slot, base)
    row_index = jnp.where(rr < region, rr, region + base + slot_index)
    count = count_ref[0]
    live_lane = f * edges + iota((1, edges), 1) < count
    row_index = jnp.where(live_lane, row_index, -1)

    def down(index):
        wide = jnp.broadcast_to(index.astype(F32), (128, edges))
        return wide.T.astype(jnp.int32)

    def select(column, first, many):
        pieces = []
        for k in range(0, many, 128):
            w = min(128, many - k)
            pieces.append((column == iota((edges, 128), 1) + (first + k)).astype(F32).astype(BF16)[:, :w])
        return jnp.concatenate(pieces, axis=1) if len(pieces) > 1 else pieces[0]

    def list_rows(d, rows):
        index = list_ref[0, pl.ds(lax.rem(g + groups - d, groups), 1), :]
        return (iota((region, slot), 0) == index).astype(F32)[:, :rows]

    for d, first, rows in blocks:
        index = list_ref[0, pl.ds(lax.rem(g + groups - d, groups), 1), :].astype(F32)
        wide = jnp.broadcast_to(index, (128, slot)).T[:rows, :]
        for k in range(0, region, 128):
            w = min(128, region - k)
            hit = wide == (iota((rows, 128), 1) + k).astype(F32)
            list_sel[first:first + rows, k:k + w] = hit.astype(F32).astype(BF16)[:, :w]

    pl.semaphore_wait(barrier, feats - 1 + groups - 1)

    own_copy = pltpu.make_async_remote_copy(
        nf, tab.at[own_rows, :], ag_s.at[0], ag_r.at[0], device_id=to(g, partner), device_id_type=MESH)
    chip_copies = []
    for j in range(1, chips):
        for rel in range(2):
            hh = h if rel == 0 else other
            cols = mine if rel == 0 else theirs
            k = 1 + (j - 1) * 2 + rel
            chip_copies.append(pltpu.make_async_remote_copy(
                nf.at[:, cols], tab.at[own_rows, cols], ag_s.at[k], ag_r.at[k],
                device_id=to(g, lax.rem(chip + j, chips) * 2 + hh), device_id_type=MESH))
    for c in chip_copies:
        c.start()
    own_copy.start()

    for c in chip_copies:
        c.wait_recv()
    own_copy.wait_recv()
    relays = []
    for j in range(1, chips):
        at = tab.at[pl.ds(pl.multiple_of(lax.rem(chip + chips - j, chips) * 2 * n_own, 2 * n_own), 2 * n_own), mine]
        relays.append(pltpu.make_async_remote_copy(
            at, at, rel_s.at[j - 1], rel_r.at[j - 1], device_id=to(g, partner), device_id_type=MESH))

    lst[...] = dot(list_sel[...], tab[0:region, mine]).astype(BF16)
    halo_copies = {}
    for i in order:
        d, first, rows = blocks[i]
        halo_copies[i] = pltpu.make_async_remote_copy(
            lst.at[first:first + rows, :], halo.at[first:first + rows, mine], h_s.at[i], h_r.at[i],
            device_id=to(lax.rem(g + groups - d, groups), f), device_id_type=MESH)
        halo_copies[i].start()
    for c in relays:
        c.start()

    sender_sel = select(down(send_ref[...]), 0, region)
    column = down(row_index)
    recv_sel[...] = select(column, 0, region + listed)
    recv_selT[...] = (iota((region + listed, edges), 0) == row_index).astype(F32).astype(BF16)
    for d, first, rows in blocks:
        list_selT[:, first:first + rows] = list_rows(d, rows).astype(BF16)

    for c in relays:
        c.wait_recv()
    loads[5].wait()
    loads[6].wait()
    pre[...] = (
        dot(ef[...], w1[0:width, :])
        + dot(dot(sender_sel, tab[0:region, :]).astype(BF16), w1[width:2 * width, :])
        + dot(dot(recv_sel[:, 0:region], tab[0:region, :]).astype(BF16), w1[2 * width:3 * width, :]))

    share = {}
    for i in order:
        d, first, rows = blocks[i]
        halo_copies[i].wait_recv()
        at = halo.at[first:first + rows, mine]
        share[i] = pltpu.make_async_remote_copy(
            at, at, hr_s.at[i], hr_r.at[i], device_id=to(g, partner), device_id_type=MESH)
        share[i].start()
    for i in order:
        share[i].wait_recv()

    for load in loads[7:10]:
        load.wait()
    table = halo[...]
    gain, shift = eg[...].astype(F32).reshape(1, width), es[...].astype(F32).reshape(1, width)
    step = edges // 2
    for k in range(0, edges, step):
        rows = slice(k, k + step)
        v = pre[rows, :] + dot(dot(recv_sel[rows, region:region + listed], table).astype(BF16), w1[2 * width:3 * width, :])
        y = dot(silu(v).astype(BF16), w2[...])
        feats_in = ef[rows, :].astype(F32)
        update = feats_in + layer_norm(y, gain, shift)
        live = f * edges + k + iota((step, 1), 0) < count
        oute[rows, :] = jnp.where(live, update, feats_in).astype(BF16)

    bounds = ((region, region + listed), (0, region))
    pairs = []
    for i, (lo, hi) in enumerate(bounds):
        pair_out[lo:hi, :] = dot(recv_selT[lo:hi, :], oute[:, theirs]).astype(BF16)
        pairs.append(pltpu.make_async_remote_copy(
            pair_out.at[lo:hi, :], pair.at[lo:hi, :], p_s.at[i], p_r.at[i],
            device_id=to(g, partner), device_id_type=MESH))
        pairs[i].start()
        if i == 0:
            part[lo:hi, :] = dot(recv_selT[lo:hi, :], oute[:, mine])
    first_pair, second_pair = pairs

    first_pair.wait_recv()
    for c in halo_copies.values():
        c.wait_send()
    lst[...] = (part[region:region + listed, :] + pair[region:region + listed, :].astype(F32)).astype(BF16)
    back = {}
    for i in order:
        d, first, rows = blocks[i]
        back[i] = pltpu.make_async_remote_copy(
            lst.at[first:first + rows, :], ret.at[first:first + rows, :], b_s.at[i], b_r.at[i],
            device_id=to(lax.rem(g + d, groups), f), device_id_type=MESH)
        back[i].start()

    part[0:region, :] = dot(recv_selT[0:region, :], oute[:, mine])
    for load in loads[10:14]:
        load.wait()
    node_in = nf[...]
    node_pre = dot(node_in, n1[0:width, :])
    second_pair.wait_recv()
    part[0:region, :] += pair[0:region, :].astype(F32)
    for i in order:
        back[i].wait_recv()
    total = part[0:region, :] + dot(list_selT[...], ret[...])
    own16[...] = total.astype(BF16)
    part[0:region, :] = total

    crosses = []
    for k in range(1, feats):
        target = lax.rem(f + k, feats)
        crosses.append(pltpu.make_async_remote_copy(
            own16.at[pl.ds(pl.multiple_of(target * n_own, n_own), n_own), :], sums.at[k - 1],
            x_s.at[k - 1], x_r.at[k - 1], device_id=to(g, target), device_id_type=MESH))
        crosses[-1].start()
    for c in crosses:
        c.wait_recv()
    kept, given = part[own_rows, :], None
    for k in range(1, feats):
        rows = sums[k - 1].astype(F32)
        if k % 2 == 0:
            kept = kept + rows
        else:
            given = rows if given is None else given + rows
    first_w = pl.ds(pl.multiple_of(width + h * half, half), half)
    second_w = pl.ds(pl.multiple_of(width + other * half, half), half)
    node_pre = node_pre + dot(kept.astype(BF16), n1[first_w, :]) + dot(given.astype(BF16), n1[second_w, :])
    node_out = dot(silu(node_pre).astype(BF16), n2[...])
    outn[...] = (node_in.astype(F32) + layer_norm(node_out, ng[...].astype(F32).reshape(1, width), ns[...].astype(F32).reshape(1, width))).astype(BF16)

    own_copy.wait_send()
    for c in chip_copies + relays + list(share.values()) + [first_pair, second_pair]:
        c.wait_send()
    for c in list(back.values()) + crosses:
        c.wait_send()


def per_device(node_feats, edge_feats, senders, receiver_ref, send_list, edge_count,
               edge_w1, edge_w2, edge_gain, edge_shift, node_w1, node_w2, node_gain, node_shift):
    groups = lax.axis_size("graph")
    feats = lax.axis_size("feat")
    n_own, width = node_feats.shape
    edges = edge_feats.shape[0]
    slot = send_list.shape[2]
    half = width // 2
    region = n_own * feats
    blocks = groups - 1
    listed = 2 * REACH * slot + (groups - 1 - 2 * REACH) * FAR_SLOT
    chips = feats // 2
    vmem = pl.BlockSpec(memory_space=pltpu.VMEM)
    hbm = pl.BlockSpec(memory_space=pl.ANY)
    dma = lambda n: pltpu.SemaphoreType.DMA((n,))
    links = 2 * max(chips - 1, 0) + 1
    return pl.pallas_call(
        functools.partial(kernel, groups, feats),
        out_shape=(pltpu.VMEM((edges, width), BF16), pltpu.VMEM((n_own, width), BF16)),
        in_specs=[hbm] * 14,
        out_specs=(vmem, vmem),
        scratch_shapes=[
            pltpu.SMEM(edge_count.shape, jnp.int32), pltpu.VMEM(node_feats.shape, BF16),
            pltpu.VMEM((1, edges), jnp.int32), pltpu.VMEM((1, edges), jnp.int32), pltpu.VMEM(send_list.shape, jnp.int32),
        ] + [pltpu.VMEM((width,), BF16)] * 4 + [
            pltpu.VMEM(edge_feats.shape, BF16), pltpu.VMEM(edge_w1.shape, BF16), pltpu.VMEM(edge_w2.shape, BF16),
            pltpu.VMEM(node_w1.shape, BF16), pltpu.VMEM(node_w2.shape, BF16),
            pltpu.VMEM((region, width), BF16),
            pltpu.VMEM((listed, half), BF16),
            pltpu.VMEM((listed + region, half), F32),
            pltpu.VMEM((listed + region, half), BF16),
            pltpu.VMEM((listed, width), BF16),
            pltpu.VMEM((listed, half), BF16),
            pltpu.VMEM((listed + region, half), BF16),
            pltpu.VMEM((region, half), BF16),
            pltpu.VMEM((feats - 1, n_own, half), BF16),
            pltpu.VMEM((edges, edge_w1.shape[1]), F32),
            pltpu.VMEM((listed, region), BF16),
            pltpu.VMEM((region, listed), BF16),
            pltpu.VMEM((edges, region + listed), BF16),
            pltpu.VMEM((region + listed, edges), BF16),
            dma(14),
            dma(links), dma(links), dma(chips - 1), dma(chips - 1),
            dma(blocks), dma(blocks), dma(blocks), dma(blocks),
            dma(2), dma(2), dma(blocks), dma(blocks), dma(feats - 1), dma(feats - 1),
        ],
        compiler_params=pltpu.CompilerParams(
            collective_id=0, has_side_effects=True, vmem_limit_bytes=60 * 1024 * 1024),
    )(edge_count, node_feats, senders.reshape(1, edges), receiver_ref.reshape(1, edges), send_list,
      edge_gain, edge_shift, node_gain, node_shift,
      edge_feats, edge_w1, edge_w2, node_w1, node_w2)


def solution(mesh):
    whole = P()
    rows = P(("graph", "feat"), None)
    flat = P(("graph", "feat"))
    return jax.shard_map(
        per_device,
        mesh=mesh,
        in_specs=(rows, rows, flat, flat, P("graph", None, None), P("graph")) + (whole,) * 8,
        out_specs=(rows, rows),
        check_vma=False,
    )
```
